32 devices in a mesh: mem: 4 (over z), lat: 2 (over y), lon: 4 (over x, core).
Axes of the slice: x: 2, y: 2, z: 4, core: 2. Of those that a mesh axis runs over, the one named last changes fastest.
Arguments:
- perturbations: bfloat16 [16, 8, 128, 1024], P('mem', None, 'lat', 'lon'), may hold values from -6 to 6
- increment: float32 [8, 128, 1024], P(None, 'lat', 'lon'), may hold values from -6 to 6
- taper_norm: float32 [8, 128, 1024], P(None, 'lat', 'lon'), may hold values from 1.5 to 6
- kappa: float32 [8], replicated, may hold values from 0.3 to 8
Outputs:
- covariance_product: float32 [8, 128, 1024], P('mem', 'lat', 'lon')
The draws below stay inside these ranges and needn't reach their ends.
All inputs are finite; a program needn't handle non-finite values.
Results may differ from the reference program's by a relative error of at most 0.0003.
Values may be sent and summed in bfloat16 or wider, within the bound.
A program may use at most 64 MiB of HBM per device.

```python
import math
import jax
import jax.numpy as jnp
from jax import lax

LEV = 8
PASSES = 4
SWEEPS = 2
MEMBERS = 16
NLAT = 128
NLON = 1024


def steps_of(rng, extent, split, least, largest):
    def one(dim, blocks):
        draws = jax.random.uniform(jax.random.fold_in(jax.random.fold_in(rng, 6), dim), (blocks,), jnp.float32, least / len(split), largest / len(split))
        return jnp.repeat(jnp.exp(draws), extent[dim] // blocks).reshape((-1,) + (1,) * (len(extent) - dim - 1))

    factor_of = one(*split[0])
    for cut in split[1:]:
        factor_of = factor_of * one(*cut)
    return factor_of


def centred(own_key, dims, deviation, reach, pieces=(), dtype=jnp.bfloat16):
    array = deviation * jax.random.normal(own_key, dims, jnp.float32)
    if pieces:
        array = array * steps_of(own_key, dims, pieces, -0.22, 0.18)
    return jnp.clip(array, -reach, reach).astype(dtype)


def setup_inputs(seed: int = 0) -> dict:
    streams_of = jax.random.split(jax.random.key(seed), 5)
    return {
        "perturbations": centred(streams_of[0], (MEMBERS, LEV, NLAT, NLON), 1.0, 6.0, ((0, 4), (2, 2), (3, 4))),
        "increment": centred(streams_of[1], (LEV, NLAT, NLON), 1.0, 6.0, ((1, 2), (2, 4)), jnp.float32),
        "taper_norm": jnp.clip(jnp.exp(math.log(6.0) - 1.3862944 * jax.random.uniform(streams_of[2], (LEV, NLAT, NLON), jnp.float32) ** steps_of(streams_of[2], (LEV, NLAT, NLON), ((1, 2), (2, 4)), -0.2, 0.2)), 1.5, 6.0),
        "kappa": jnp.clip(jnp.exp(jax.random.uniform(streams_of[3], (LEV,), jnp.float32, math.log(0.3), math.log(8.0))), 0.3, 8.0),
    }


def relax_whole(source, field, weight):
    padded = jnp.pad(field, ((0, 0), (1, 1), (0, 0)))
    padded = jnp.concatenate([padded[:, :, -1:], padded, padded[:, :, :1]], axis=2)
    beside_all = padded[:, 2:, 1:-1] + padded[:, :-2, 1:-1] + padded[:, 1:-1, 2:] + padded[:, 1:-1, :-2]
    return (source + weight * beside_all) / (1.0 + 4.0 * weight)


def diffuse_whole(field, weight):
    for turn in range(2 * PASSES):
        result = field
        for sweep in range(SWEEPS):
            result = relax_whole(field, result, weight)
        field = result
    return field


def reference(perturbations, increment, taper_norm, kappa):
    weight = kappa[:, None, None]

    def add_member(total, member):
        values = member.astype(jnp.float32)
        spread = taper_norm * (values * increment)
        tapered = taper_norm * diffuse_whole(spread, weight)
        return total + values * tapered, None

    total, unused = lax.scan(add_member, jnp.zeros(increment.shape, jnp.float32), perturbations)
    return total / (MEMBERS - 1)
```

```python
import functools

import jax
import jax.numpy as jnp
from jax import lax
from jax.experimental import pallas as pl
from jax.experimental.pallas import tpu as pltpu
from jax.sharding import PartitionSpec as P

PASSES = 4
SWEEPS = 2
DEPTH = 2 * PASSES * SWEEPS
SUB = 8
LANES = 128
MESH = pl.DeviceIdType.MESH


def roll(value, shift):
    shift = shift % LANES
    return value if shift == 0 else pltpu.roll(value, shift, value.ndim - 1)


def kernel(
    sizes, kappa, pert, inc, taper, out,
    g, pack, rlon, cpack, rcor, rlat_p, rlat_g, nat, xs, ys, zs, part, rpart,
    lon_send, lon_recv, latp_send, latp_recv, latg_send, latg_recv,
    cor_send, cor_recv, part_send, part_recv,
):
    n_mem, n_lat, n_lon = sizes
    members, levels, rows, cols = pert.shape
    per = levels // n_mem
    pitch = nat.shape[1] // SUB
    step = (cols + 2 * DEPTH - LANES) // 2
    span = rows + (DEPTH if n_lat == 2 else 2 * DEPTH if n_lat > 2 else 0)
    mem, lat, lon = lax.axis_index("mem"), lax.axis_index("lat"), lax.axis_index("lon")
    base = 1 + jnp.where(lat == 0, DEPTH, 0) if n_lat <= 2 else 1
    lane = lax.broadcasted_iota(jnp.int32, (SUB, LANES), 1)
    sub = lax.broadcasted_iota(jnp.int32, (SUB, LANES), 0)
    lon_to = [lax.rem(lon + 1, n_lon), lax.rem(lon + n_lon - 1, n_lon)]
    lat_to = [lat + 1, lat - 1]
    sends = [lat < n_lat - 1, lat > 0]
    gets = [lat > 0, lat < n_lat - 1]
    edge = [rows - DEPTH, 0]

    def group(t):
        return lax.rem(mem + 1 + t, n_mem)

    def remote(src, dst, send, recv, **where):
        return pltpu.make_async_remote_copy(
            src_ref=src, dst_ref=dst, send_sem=send, recv_sem=recv,
            device_id=where, device_id_type=MESH,
        )

    def lon_copy(t, b):
        return remote(pack.at[b, t], rlon.at[b, t], lon_send.at[b, t], lon_recv.at[b, t],
                      mem=mem, lat=lat, lon=lon_to[b])

    def cor_copy(t, a, b):
        return remote(cpack.at[a, b, t], rcor.at[a, b, t], cor_send.at[a, b, t],
                      cor_recv.at[a, b, t], mem=mem, lat=lat_to[a], lon=lon_to[b])

    def latp_copy(t, a):
        return remote(pert.at[:, pl.ds(group(t) * per, per), pl.ds(edge[a], DEPTH), :],
                      rlat_p.at[a, t], latp_send.at[a, t], latp_recv.at[a, t],
                      mem=mem, lat=lat_to[a], lon=lon)

    def latg_copy(t, a):
        return remote(g.at[pl.ds(group(t) * per, per), pl.ds(edge[a], DEPTH), :],
                      rlat_g.at[a, t], latg_send.at[a, t], latg_recv.at[a, t],
                      mem=mem, lat=lat_to[a], lon=lon)

    def part_copy(t):
        return remote(part.at[t], rpart.at[t], part_send.at[t], part_recv.at[t],
                      mem=group(t), lat=lat, lon=lon)

    barrier = pltpu.get_barrier_semaphore()

    def greet(**where):
        pl.semaphore_signal(barrier, inc=1, device_id=where, device_id_type=MESH)

    for b in range(2):
        greet(mem=mem, lat=lat, lon=lon_to[b])
    for t in range(n_mem - 1):
        greet(mem=group(t), lat=lat, lon=lon)
    for a in range(2):
        @pl.when(sends[a])
        def _():
            greet(mem=mem, lat=lat_to[a], lon=lon)
            for b in range(2):
                greet(mem=mem, lat=lat_to[a], lon=lon_to[b])

    g[...] = taper[...] * inc[...]
    for buf in (xs, ys, zs):
        buf[...] = jnp.zeros_like(buf)

    beside = sum(jnp.where(s, 1, 0) for s in sends)
    pl.semaphore_wait(barrier, 2 + (n_mem - 1) + 3 * beside)

    def send_group(t, carry):
        e = group(t)
        for a in range(2):
            @pl.when(sends[a])
            def _():
                latg_copy(t, a).start()
                latp_copy(t, a).start()
        for b, column in enumerate((cols - LANES, 0)):
            source = LANES - DEPTH if b == 0 else 0
            corners = [[None] * (SUB * 2 * DEPTH // LANES) for _ in range(2)]
            for s in range(SUB):
                m, l = s // per, s % per
                w = pert[m, e * per + l, :, pl.ds(column, LANES)].astype(jnp.float32)
                w = w * g[e * per + l, :, pl.ds(column, LANES)]
                acc = None
                for q in range(rows // SUB):
                    v = roll(w[q * SUB : (q + 1) * SUB], q * DEPTH - source)
                    acc = v if acc is None else jnp.where(lane >= q * DEPTH, v, acc)
                pack[b, t, s] = acc
                each = LANES // (2 * DEPTH)
                j, i = s // each, s % each
                for a in range(2):
                    start = (edge[a] // SUB) * DEPTH
                    v = roll(acc, i * 2 * DEPTH - start)
                    old = corners[a][j]
                    corners[a][j] = v if old is None else jnp.where(lane >= i * 2 * DEPTH, v, old)
            for a in range(2):
                for j, v in enumerate(corners[a]):
                    cpack[a, b, t, j] = v
            lon_copy(t, b).start()
            for a in range(2):
                @pl.when(sends[a])
                def _():
                    cor_copy(t, a, b).start()
        return carry

    lax.fori_loop(0, n_mem, send_group, 0)

    def place(s, row, x0, x1, low, high):
        at = pl.ds(s * pitch + row, SUB)
        nat[0, at, :] = jnp.where(lane < DEPTH, low, roll(x0, DEPTH))
        cut = LANES - (step - DEPTH)
        nat[1, at, :] = jnp.where(lane < cut, roll(x0, cut), roll(x1, cut))
        nat[2, at, :] = jnp.where(lane < LANES - DEPTH, roll(x1, -DEPTH), high)

    def windows(t):
        e = group(t)
        for s in range(SUB):
            m, l = s // per, s % per
            w = pert[m, e * per + l].astype(jnp.float32) * g[e * per + l]
            left, right = rlon[0, t, s], rlon[1, t, s]
            for q in range(rows // SUB):
                r = slice(q * SUB, (q + 1) * SUB)
                place(s, DEPTH + q * SUB, w[r, :LANES], w[r, LANES:],
                      roll(left, -q * DEPTH), roll(right, LANES - DEPTH - q * DEPTH))
        each = LANES // (2 * DEPTH)
        for a in range(2):
            first = 0 if a == 0 else DEPTH + rows

            @pl.when(gets[a])
            def _():
                for s in range(SUB):
                    m, l = s // per, s % per
                    j, i = s // each, s % each
                    w = rlat_p[a, t, m, l].astype(jnp.float32) * rlat_g[a, t, l]
                    left, right = rcor[a, 0, t, j], rcor[a, 1, t, j]
                    for h in range(DEPTH // SUB):
                        r = slice(h * SUB, (h + 1) * SUB)
                        at = i * 2 * DEPTH + h * DEPTH
                        place(s, first + h * SUB, w[r, :LANES], w[r, LANES:],
                              roll(left, -at), roll(right, LANES - DEPTH - at))

            @pl.when(jnp.logical_not(gets[a]))
            def _():
                zero = jnp.zeros((DEPTH, LANES), jnp.float32)
                for s in range(SUB):
                    for k in range(3):
                        nat[k, pl.ds(s * pitch + first, DEPTH), :] = zero

    def gather(i, carry):
        for k in range(3):
            for j in range(SUB):
                r = i * SUB + j
                xs[k, 1 + r] = nat[k, pl.ds(r, SUB, stride=pitch), :]
        return carry

    def scatter(i, carry):
        for k in range(3):
            for j in range(SUB):
                r = DEPTH + i * SUB + j
                nat[k, pl.ds(r, SUB, stride=pitch), :] = xs[k, 1 + r]
        return carry

    def sweep(field, source, coef, target):
        block = SUB
        for i in range(0, span, block):
            for k in range(3):
                x = field[k, pl.ds(base + i - 1, block + 2)]
                p = x[:-1] + roll(x[1:], 1)
                p = p[:-1] + roll(p[1:], -1)
                own = x[1:-1] if source is field else source[k, pl.ds(base + i, block)]
                target[k, pl.ds(base + i, block)] = p + coef * own
        if n_lat > 2:
            for a in range(2):
                @pl.when(jnp.logical_not(gets[a]))
                def _():
                    for k in range(3):
                        target[k, pl.ds(1 if a == 0 else 1 + DEPTH + rows, DEPTH)] = jnp.zeros(
                            (DEPTH, SUB, LANES), jnp.float32)

    def work(t, carry):
        e = group(t)
        for b in range(2):
            lon_copy(t, b).wait_recv()
        for a in range(2):
            @pl.when(gets[a])
            def _():
                latg_copy(t, a).wait_recv()
                latp_copy(t, a).wait_recv()
                for b in range(2):
                    cor_copy(t, a, b).wait_recv()
        windows(t)
        lax.fori_loop(0, (rows + 2 * DEPTH) // SUB, gather, 0)
        weight = jnp.zeros((SUB, LANES), jnp.float32)
        for s in range(SUB):
            weight = jnp.where(sub == s, kappa[e * per + s % per], weight)
        first = 1.0 / weight
        second = first * (4.0 + first)

        def two(i, c):
            sweep(xs, xs, first, ys)
            sweep(ys, xs, second, zs)
            sweep(zs, zs, first, ys)
            sweep(ys, zs, second, xs)
            return c

        lax.fori_loop(0, PASSES, two, 0)
        lax.fori_loop(0, rows // SUB, scatter, 0)
        cut = LANES - (step - DEPTH)
        for l in range(per):
            k1 = jnp.full((SUB, LANES), kappa[e * per + l], jnp.float32)
            factor = k1 / (1.0 + 4.0 * k1)
            power = jnp.ones_like(factor)
            for _ in range(2 * PASSES * SWEEPS):
                power = power * factor
            factor = power / (members * n_mem - 1)
            for q in range(0, rows, 2 * SUB):
                sums = [[0.0, 0.0], [0.0, 0.0]]
                for m in range(members):
                    s = m * per + l
                    v = pert[m, e * per + l, q : q + 2 * SUB, :].astype(jnp.float32)
                    for h in range(2):
                        at = pl.ds(s * pitch + DEPTH + q + h * SUB, SUB)
                        mid = roll(nat[1, at, :], cut)
                        low = jnp.where(lane < LANES - 2 * DEPTH, roll(nat[0, at, :], -DEPTH), mid)
                        high = jnp.where(lane < cut - DEPTH, mid, roll(nat[2, at, :], DEPTH))
                        r = slice(h * SUB, (h + 1) * SUB)
                        sums[h][0] = sums[h][0] + v[r, :LANES] * low
                        sums[h][1] = sums[h][1] + v[r, LANES:] * high
                for h in range(2):
                    at = pl.ds(q + h * SUB, SUB)
                    tap = taper[e * per + l, at, :]
                    part[t, l, at, :LANES] = sums[h][0] * tap[:, :LANES] * factor
                    part[t, l, at, LANES:] = sums[h][1] * tap[:, LANES:] * factor

        @pl.when(t < n_mem - 1)
        def _():
            part_copy(t).start()

        return carry

    lax.fori_loop(0, n_mem, work, 0)
    total = part[n_mem - 1]
    for t in range(n_mem - 1):
        part_copy(t).wait_recv()
        total = total + rpart[t]
    out[...] = total

    def drain(t, carry):
        for b in range(2):
            lon_copy(t, b).wait_send()
        for a in range(2):
            @pl.when(sends[a])
            def _():
                latg_copy(t, a).wait_send()
                latp_copy(t, a).wait_send()
                for b in range(2):
                    cor_copy(t, a, b).wait_send()
        return carry

    lax.fori_loop(0, n_mem, drain, 0)
    for t in range(n_mem - 1):
        part_copy(t).wait_send()


def local(sizes, perturbations, increment, taper_norm, kappa):
    n_mem, n_lat, n_lon = sizes
    members, levels, rows, cols = perturbations.shape
    per = levels // n_mem
    assert members * per == SUB and cols == 2 * LANES and rows * DEPTH == SUB * LANES
    f32 = jnp.float32
    full = rows + 2 * DEPTH
    pitch = full + SUB // 2
    tiles = SUB * 2 * DEPTH // LANES
    field = pltpu.VMEM((3, full + 2, SUB, LANES), f32)
    dma = pltpu.SemaphoreType.DMA
    vmem = pl.BlockSpec(memory_space=pltpu.VMEM)
    return pl.pallas_call(
        functools.partial(kernel, sizes),
        out_shape=jax.ShapeDtypeStruct((per, rows, cols), f32),
        in_specs=[pl.BlockSpec(memory_space=pltpu.SMEM), vmem, vmem, vmem],
        out_specs=vmem,
        scratch_shapes=[
            pltpu.VMEM((levels, rows, cols), f32),
            pltpu.VMEM((2, n_mem, SUB, SUB, LANES), f32),
            pltpu.VMEM((2, n_mem, SUB, SUB, LANES), f32),
            pltpu.VMEM((2, 2, n_mem, tiles, SUB, LANES), f32),
            pltpu.VMEM((2, 2, n_mem, tiles, SUB, LANES), f32),
            pltpu.VMEM((2, n_mem, members, per, DEPTH, cols), jnp.bfloat16),
            pltpu.VMEM((2, n_mem, per, DEPTH, cols), f32),
            pltpu.VMEM((3, SUB * pitch, LANES), f32),
            field, field, field,
            pltpu.VMEM((n_mem, per, rows, cols), f32),
            pltpu.VMEM((n_mem - 1, per, rows, cols), f32),
            dma((2, n_mem)), dma((2, n_mem)),
            dma((2, n_mem)), dma((2, n_mem)),
            dma((2, n_mem)), dma((2, n_mem)),
            dma((2, 2, n_mem)), dma((2, 2, n_mem)),
            dma((n_mem - 1,)), dma((n_mem - 1,)),
        ],
        compiler_params=pltpu.CompilerParams(collective_id=0, has_side_effects=True),
    )(kappa, perturbations, increment, taper_norm)


def solution(mesh):
    sizes = tuple(mesh.shape[name] for name in ("mem", "lat", "lon"))
    return jax.shard_map(
        functools.partial(local, sizes),
        mesh=mesh,
        in_specs=(P("mem", None, "lat", "lon"), P(None, "lat", "lon"), P(None, "lat", "lon"), P()),
        out_specs=P("mem", "lat", "lon"),
        check_vma=False,
    )
```

```python
import functools

import jax
import jax.numpy as jnp
from jax import lax
from jax.experimental import pallas as pl
from jax.experimental.pallas import tpu as pltpu
from jax.sharding import PartitionSpec as P

PASSES = 4
SWEEPS = 2
DEPTH = 2 * PASSES * SWEEPS
SUB = 8
LANES = 128
MESH = pl.DeviceIdType.MESH


def roll(value, shift):
    shift = shift % LANES
    return value if shift == 0 else pltpu.roll(value, shift, value.ndim - 1)


def kernel(
    sizes, kappa, pert, inc, taper, out,
    g, pack, rlon, cpack, rcor, rlat_p, rlat_g, nat, xs, ys, zs, part, rpart,
    lon_send, lon_recv, latp_send, latp_recv, latg_send, latg_recv,
    cor_send, cor_recv, part_send, part_recv,
):
    n_mem, n_lat, n_lon = sizes
    members, levels, rows, cols = pert.shape
    per = levels // n_mem
    pitch = nat.shape[1] // SUB
    step = (cols + 2 * DEPTH - LANES) // 2
    span = rows + (DEPTH if n_lat == 2 else 2 * DEPTH if n_lat > 2 else 0)
    mem, lat, lon = lax.axis_index("mem"), lax.axis_index("lat"), lax.axis_index("lon")
    base = 1 + jnp.where(lat == 0, DEPTH, 0) if n_lat <= 2 else 1
    lane = lax.broadcasted_iota(jnp.int32, (SUB, LANES), 1)
    sub = lax.broadcasted_iota(jnp.int32, (SUB, LANES), 0)
    lon_to = [lax.rem(lon + 1, n_lon), lax.rem(lon + n_lon - 1, n_lon)]
    lat_to = [lat + 1, lat - 1]
    sends = [lat < n_lat - 1, lat > 0]
    gets = [lat > 0, lat < n_lat - 1]
    edge = [rows - DEPTH, 0]

    def group(t):
        return lax.rem(mem + 1 + t, n_mem)

    def remote(src, dst, send, recv, **where):
        return pltpu.make_async_remote_copy(
            src_ref=src, dst_ref=dst, send_sem=send, recv_sem=recv,
            device_id=where, device_id_type=MESH,
        )

    def lon_copy(t, b):
        return remote(pack.at[b, t], rlon.at[b, t], lon_send.at[b, t], lon_recv.at[b, t],
                      mem=mem, lat=lat, lon=lon_to[b])

    def cor_copy(t, a, b):
        return remote(cpack.at[a, b, t], rcor.at[a, b, t], cor_send.at[a, b, t],
                      cor_recv.at[a, b, t], mem=mem, lat=lat_to[a], lon=lon_to[b])

    def latp_copy(t, a):
        return remote(pert.at[:, pl.ds(group(t) * per, per), pl.ds(edge[a], DEPTH), :],
                      rlat_p.at[a, t], latp_send.at[a, t], latp_recv.at[a, t],
                      mem=mem, lat=lat_to[a], lon=lon)

    def latg_copy(t, a):
        return remote(g.at[pl.ds(group(t) * per, per), pl.ds(edge[a], DEPTH), :],
                      rlat_g.at[a, t], latg_send.at[a, t], latg_recv.at[a, t],
                      mem=mem, lat=lat_to[a], lon=lon)

    def part_copy(t):
        return remote(part.at[t], rpart.at[t], part_send.at[t], part_recv.at[t],
                      mem=group(t), lat=lat, lon=lon)

    barrier = pltpu.get_barrier_semaphore()

    def greet(**where):
        pl.semaphore_signal(barrier, inc=1, device_id=where, device_id_type=MESH)

    for b in range(2):
        greet(mem=mem, lat=lat, lon=lon_to[b])
    for t in range(n_mem - 1):
        greet(mem=group(t), lat=lat, lon=lon)
    for a in range(2):
        @pl.when(sends[a])
        def _():
            greet(mem=mem, lat=lat_to[a], lon=lon)
            for b in range(2):
                greet(mem=mem, lat=lat_to[a], lon=lon_to[b])

    g[...] = taper[...] * inc[...]
    for buf in (xs, ys, zs):
        buf[...] = jnp.zeros_like(buf)

    beside = sum(jnp.where(s, 1, 0) for s in sends)
    pl.semaphore_wait(barrier, 2 + (n_mem - 1) + 3 * beside)

    def send_group(t, carry):
        e = group(t)
        for a in range(2):
            @pl.when(sends[a])
            def _():
                latg_copy(t, a).start()
                latp_copy(t, a).start()
        for b, column in enumerate((cols - LANES, 0)):
            source = LANES - DEPTH if b == 0 else 0
            corners = [[None] * (SUB * 2 * DEPTH // LANES) for _ in range(2)]
            for s in range(SUB):
                m, l = s // per, s % per
                w = pert[m, e * per + l, :, pl.ds(column, LANES)].astype(jnp.float32)
                w = w * g[e * per + l, :, pl.ds(column, LANES)]
                acc = None
                for q in range(rows // SUB):
                    v = roll(w[q * SUB : (q + 1) * SUB], q * DEPTH - source)
                    acc = v if acc is None else jnp.where(lane >= q * DEPTH, v, acc)
                pack[b, t, s] = acc
                each = LANES // (2 * DEPTH)
                j, i = s // each, s % each
                for a in range(2):
                    start = (edge[a] // SUB) * DEPTH
                    v = roll(acc, i * 2 * DEPTH - start)
                    old = corners[a][j]
                    corners[a][j] = v if old is None else jnp.where(lane >= i * 2 * DEPTH, v, old)
            for a in range(2):
                for j, v in enumerate(corners[a]):
                    cpack[a, b, t, j] = v
            lon_copy(t, b).start()
            for a in range(2):
                @pl.when(sends[a])
                def _():
                    cor_copy(t, a, b).start()
        return carry

    lax.fori_loop(0, n_mem, send_group, 0)

    def place(s, row, x0, x1, low, high):
        at = pl.ds(s * pitch + row, SUB)
        nat[0, at, :] = jnp.where(lane < DEPTH, low, roll(x0, DEPTH))
        cut = LANES - (step - DEPTH)
        nat[1, at, :] = jnp.where(lane < cut, roll(x0, cut), roll(x1, cut))
        nat[2, at, :] = jnp.where(lane < LANES - DEPTH, roll(x1, -DEPTH), high)

    def windows(t):
        e = group(t)
        for s in range(SUB):
            m, l = s // per, s % per
            w = pert[m, e * per + l].astype(jnp.float32) * g[e * per + l]
            left, right = rlon[0, t, s], rlon[1, t, s]
            for q in range(rows // SUB):
                r = slice(q * SUB, (q + 1) * SUB)
                place(s, DEPTH + q * SUB, w[r, :LANES], w[r, LANES:],
                      roll(left, -q * DEPTH), roll(right, LANES - DEPTH - q * DEPTH))
        each = LANES // (2 * DEPTH)
        for a in range(2):
            first = 0 if a == 0 else DEPTH + rows

            @pl.when(gets[a])
            def _():
                for s in range(SUB):
                    m, l = s // per, s % per
                    j, i = s // each, s % each
                    w = rlat_p[a, t, m, l].astype(jnp.float32) * rlat_g[a, t, l]
                    left, right = rcor[a, 0, t, j], rcor[a, 1, t, j]
                    for h in range(DEPTH // SUB):
                        r = slice(h * SUB, (h + 1) * SUB)
                        at = i * 2 * DEPTH + h * DEPTH
                        place(s, first + h * SUB, w[r, :LANES], w[r, LANES:],
                              roll(left, -at), roll(right, LANES - DEPTH - at))

            @pl.when(jnp.logical_not(gets[a]))
            def _():
                zero = jnp.zeros((DEPTH, LANES), jnp.float32)
                for s in range(SUB):
                    for k in range(3):
                        nat[k, pl.ds(s * pitch + first, DEPTH), :] = zero

    def gather(i, carry):
        for k in range(3):
            for j in range(SUB):
                r = i * SUB + j
                xs[k, 1 + r] = nat[k, pl.ds(r, SUB, stride=pitch), :]
        return carry

    def scatter(i, carry):
        for k in range(3):
            for j in range(SUB):
                r = DEPTH + i * SUB + j
                nat[k, pl.ds(r, SUB, stride=pitch), :] = xs[k, 1 + r]
        return carry

    def sweep(field, source, coef, target):
        block = SUB
        for i in range(0, span, block):
            for k in range(3):
                x = field[k, pl.ds(base + i - 1, block + 2)]
                mid = x[1:-1]
                own = mid if source is field else source[k, pl.ds(base + i, block)]
                beside = roll(mid, 1) + roll(mid, -1)
                target[k, pl.ds(base + i, block)] = (x[2:] + x[:-2]) + coef * own + beside
        if n_lat > 2:
            for a in range(2):
                @pl.when(jnp.logical_not(gets[a]))
                def _():
                    for k in range(3):
                        target[k, pl.ds(1 if a == 0 else 1 + DEPTH + rows, DEPTH)] = jnp.zeros(
                            (DEPTH, SUB, LANES), jnp.float32)

    def work(t, carry):
        e = group(t)
        for b in range(2):
            lon_copy(t, b).wait_recv()
        for a in range(2):
            @pl.when(gets[a])
            def _():
                latg_copy(t, a).wait_recv()
                latp_copy(t, a).wait_recv()
                for b in range(2):
                    cor_copy(t, a, b).wait_recv()
        windows(t)
        lax.fori_loop(0, (rows + 2 * DEPTH) // SUB, gather, 0)
        weight = jnp.zeros((SUB, LANES), jnp.float32)
        for s in range(SUB):
            weight = jnp.where(sub == s, kappa[e * per + s % per], weight)
        first = 1.0 / weight
        second = first * (4.0 + first)

        def two(i, c):
            sweep(xs, xs, first, ys)
            sweep(ys, xs, second, zs)
            sweep(zs, zs, first, ys)
            sweep(ys, zs, second, xs)
            return c

        lax.fori_loop(0, PASSES, two, 0)
        lax.fori_loop(0, rows // SUB, scatter, 0)
        cut = LANES - (step - DEPTH)
        for l in range(per):
            k1 = jnp.full((SUB, LANES), kappa[e * per + l], jnp.float32)
            factor = k1 / (1.0 + 4.0 * k1)
            power = jnp.ones_like(factor)
            for _ in range(2 * PASSES * SWEEPS):
                power = power * factor
            factor = power / (members * n_mem - 1)
            for q in range(0, rows, 2 * SUB):
                sums = [[0.0, 0.0], [0.0, 0.0]]
                for m in range(members):
                    s = m * per + l
                    v = pert[m, e * per + l, q : q + 2 * SUB, :].astype(jnp.float32)
                    for h in range(2):
                        at = pl.ds(s * pitch + DEPTH + q + h * SUB, SUB)
                        mid = roll(nat[1, at, :], cut)
                        low = jnp.where(lane < LANES - 2 * DEPTH, roll(nat[0, at, :], -DEPTH), mid)
                        high = jnp.where(lane < cut - DEPTH, mid, roll(nat[2, at, :], DEPTH))
                        r = slice(h * SUB, (h + 1) * SUB)
                        sums[h][0] = sums[h][0] + v[r, :LANES] * low
                        sums[h][1] = sums[h][1] + v[r, LANES:] * high
                for h in range(2):
                    at = pl.ds(q + h * SUB, SUB)
                    tap = taper[e * per + l, at, :]
                    part[t, l, at, :LANES] = sums[h][0] * tap[:, :LANES] * factor
                    part[t, l, at, LANES:] = sums[h][1] * tap[:, LANES:] * factor

        @pl.when(t < n_mem - 1)
        def _():
            part_copy(t).start()

        return carry

    lax.fori_loop(0, n_mem, work, 0)
    total = part[n_mem - 1]
    for t in range(n_mem - 1):
        part_copy(t).wait_recv()
        total = total + rpart[t]
    out[...] = total

    def drain(t, carry):
        for b in range(2):
            lon_copy(t, b).wait_send()
        for a in range(2):
            @pl.when(sends[a])
            def _():
                latg_copy(t, a).wait_send()
                latp_copy(t, a).wait_send()
                for b in range(2):
                    cor_copy(t, a, b).wait_send()
        return carry

    lax.fori_loop(0, n_mem, drain, 0)
    for t in range(n_mem - 1):
        part_copy(t).wait_send()


def local(sizes, perturbations, increment, taper_norm, kappa):
    n_mem, n_lat, n_lon = sizes
    members, levels, rows, cols = perturbations.shape
    per = levels // n_mem
    assert members * per == SUB and cols == 2 * LANES and rows * DEPTH == SUB * LANES
    f32 = jnp.float32
    full = rows + 2 * DEPTH
    pitch = full + SUB // 2
    tiles = SUB * 2 * DEPTH // LANES
    field = pltpu.VMEM((3, full + 2, SUB, LANES), f32)
    dma = pltpu.SemaphoreType.DMA
    vmem = pl.BlockSpec(memory_space=pltpu.VMEM)
    return pl.pallas_call(
        functools.partial(kernel, sizes),
        out_shape=jax.ShapeDtypeStruct((per, rows, cols), f32),
        in_specs=[pl.BlockSpec(memory_space=pltpu.SMEM), vmem, vmem, vmem],
        out_specs=vmem,
        scratch_shapes=[
            pltpu.VMEM((levels, rows, cols), f32),
            pltpu.VMEM((2, n_mem, SUB, SUB, LANES), f32),
            pltpu.VMEM((2, n_mem, SUB, SUB, LANES), f32),
            pltpu.VMEM((2, 2, n_mem, tiles, SUB, LANES), f32),
            pltpu.VMEM((2, 2, n_mem, tiles, SUB, LANES), f32),
            pltpu.VMEM((2, n_mem, members, per, DEPTH, cols), jnp.bfloat16),
            pltpu.VMEM((2, n_mem, per, DEPTH, cols), f32),
            pltpu.VMEM((3, SUB * pitch, LANES), f32),
            field, field, field,
            pltpu.VMEM((n_mem, per, rows, cols), f32),
            pltpu.VMEM((n_mem - 1, per, rows, cols), f32),
            dma((2, n_mem)), dma((2, n_mem)),
            dma((2, n_mem)), dma((2, n_mem)),
            dma((2, n_mem)), dma((2, n_mem)),
            dma((2, 2, n_mem)), dma((2, 2, n_mem)),
            dma((n_mem - 1,)), dma((n_mem - 1,)),
        ],
        compiler_params=pltpu.CompilerParams(collective_id=0, has_side_effects=True),
    )(kappa, perturbations, increment, taper_norm)


def solution(mesh):
    sizes = tuple(mesh.shape[name] for name in ("mem", "lat", "lon"))
    return jax.shard_map(
        functools.partial(local, sizes),
        mesh=mesh,
        in_specs=(P("mem", None, "lat", "lon"), P(None, "lat", "lon"), P(None, "lat", "lon"), P()),
        out_specs=P("mem", "lat", "lon"),
        check_vma=False,
    )
```
